32 devices in a mesh: gx: 4 (over x, core), gy: 8 (over z, y).
Axes of the slice: x: 2, y: 2, z: 4, core: 2. Of those that a mesh axis runs over, the one named last changes fastest.
Arguments:
- text_in: bfloat16 [32, 128, 768], P(('gx', 'gy')), may hold values from -6 to 6
- image_in: bfloat16 [32, 36, 1024], P(('gx', 'gy')), may hold values from -6 to 6
- text_lengths: int32 [32], P(('gx', 'gy')), may hold values from 8 to 128, as said below
- region_mask: int32 [32, 36], P(('gx', 'gy')), may hold values 0 or 1
- text_cot: bfloat16 [32, 128, 768], P(('gx', 'gy')), may hold values from -6 to 6
- image_cot: bfloat16 [32, 36, 1024], P(('gx', 'gy')), may hold values from -6 to 6
- co_text_proj: bfloat16 [3, 768, 1024], P(None, ('gx', 'gy')), may hold values from -0.21875 to 0.21875
- co_image_proj: bfloat16 [3, 1024, 1024], P(None, ('gx', 'gy')), may hold values from -0.1875 to 0.1875
- co_bias: bfloat16 [4, 1024], P(None, ('gx', 'gy')), may hold values from -3 to 3
- co_text_out: bfloat16 [1024, 768], P(('gx', 'gy')), may hold values from -0.75 to 0.75
- co_image_out: bfloat16 [1024, 1024], P(('gx', 'gy')), may hold values from -0.75 to 0.75
- text_up: bfloat16 [768, 3072], P(('gx', 'gy')), may hold values from -0.21875 to 0.21875
- text_up_bias: bfloat16 [3072], P(('gx', 'gy')), may hold values from -3 to 3
- text_down: bfloat16 [3072, 768], P(('gx', 'gy')), may hold values from -0.109375 to 0.109375
- image_up: bfloat16 [1024, 1024], P(('gx', 'gy')), may hold values from -0.1875 to 0.1875
- image_up_bias: bfloat16 [1024], P(('gx', 'gy')), may hold values from -3 to 3
- image_down: bfloat16 [1024, 1024], P(('gx', 'gy')), may hold values from -0.1875 to 0.1875
- text_self_qkv: bfloat16 [3, 768, 768], P(None, ('gx', 'gy')), may hold values from -0.21875 to 0.21875
- text_self_out: bfloat16 [768, 768], P(('gx', 'gy')), may hold values from -0.875 to 0.875
- image_self_qkv: bfloat16 [3, 1024, 1024], P(None, ('gx', 'gy')), may hold values from -0.1875 to 0.1875
- image_self_out: bfloat16 [1024, 1024], P(('gx', 'gy')), may hold values from -0.75 to 0.75
- text_gains: bfloat16 [3, 768], P(None, ('gx', 'gy')), may hold values from 0.5 to 1.5
- image_gains: bfloat16 [3, 1024], P(None, ('gx', 'gy')), may hold values from 0.5 to 1.5
- text_vectors: bfloat16 [8, 768], P(None, ('gx', 'gy')), may hold values from -3 to 3
- image_vectors: bfloat16 [8, 1024], P(None, ('gx', 'gy')), may hold values from -3 to 3
Outputs:
- text_out: bfloat16 [32, 128, 768], P(('gx', 'gy'))
- image_out: bfloat16 [32, 36, 1024], P(('gx', 'gy'))
- text_in_grad: bfloat16 [32, 128, 768], P(('gx', 'gy'))
- image_in_grad: bfloat16 [32, 36, 1024], P(('gx', 'gy'))
- co_text_proj_grad: float32 [3, 768, 1024], P(None, ('gx', 'gy'))
- co_image_proj_grad: float32 [3, 1024, 1024], P(None, ('gx', 'gy'))
- co_bias_grad: float32 [4, 1024], P(None, ('gx', 'gy'))
- co_text_out_grad: float32 [1024, 768], P(('gx', 'gy'))
- co_image_out_grad: float32 [1024, 1024], P(('gx', 'gy'))
- text_up_grad: float32 [768, 3072], P(('gx', 'gy'))
- text_up_bias_grad: float32 [3072], P(('gx', 'gy'))
- text_down_grad: float32 [3072, 768], P(('gx', 'gy'))
- image_up_grad: float32 [1024, 1024], P(('gx', 'gy'))
- image_up_bias_grad: float32 [1024], P(('gx', 'gy'))
- image_down_grad: float32 [1024, 1024], P(('gx', 'gy'))
- text_self_qkv_grad: float32 [3, 768, 768], P(None, ('gx', 'gy'))
- text_self_out_grad: float32 [768, 768], P(('gx', 'gy'))
- image_self_qkv_grad: float32 [3, 1024, 1024], P(None, ('gx', 'gy'))
- image_self_out_grad: float32 [1024, 1024], P(('gx', 'gy'))
- text_gains_grad: float32 [3, 768], P(None, ('gx', 'gy'))
- image_gains_grad: float32 [3, 1024], P(None, ('gx', 'gy'))
- text_vectors_grad: float32 [8, 768], P(None, ('gx', 'gy'))
- image_vectors_grad: float32 [8, 1024], P(None, ('gx', 'gy'))
The draws below stay inside these ranges and needn't reach their ends.
Inputs may be any that keep to these rules, and one draw needn't show every extreme that they name: `text_lengths`: some pair has exactly 128 caption tokens and some other pair exactly 8; every other pair has 80 to 128 tokens.
All inputs are finite; a program needn't handle non-finite values. No bound on the sum of `region_mask` on one device may be relied on, other than what follows from the above.
Results may differ from the reference program's by a relative error of at most 0.025.
Values may be sent and summed in bfloat16 or wider, within the bound.
A program may use at most 256 MiB of HBM per device.

```python
import math
import jax
import jax.numpy as jnp
from jax import lax

DT = 768
HT = 12
FT = 3072
DV = 1024
HV = 8
FV = 1024
CO = 1024
CHN = 8
LT = 128
LV = 36
PAIRS = 32
MIN_LEN = 8


def draw_text_lengths(key, part):
    first_key, second_key, third_key = jax.random.split(key, 3)
    lengths = jax.random.randint(first_key, (PAIRS,), 5 * LT // 8, LT + 1)
    longest = jax.random.randint(second_key, (), 0, PAIRS)
    shortest = (longest + 1 + jax.random.randint(third_key, (), 0, PAIRS - 1)) % PAIRS
    places = jnp.arange(PAIRS)
    lengths = jnp.where(places == longest, LT, lengths)
    lengths = jnp.where(places == shortest, MIN_LEN, lengths)
    return lengths.astype(jnp.int32)


def set_ends(array, stream_key, low, largest):
    longest = array.shape.index(max(array.shape))
    spots = []
    for shift in (0, 1):
        where = [jax.random.randint(jax.random.fold_in(stream_key, axis), (), 0, length) for axis, length in enumerate(array.shape)]
        where[longest] = (where[longest] + shift) % array.shape[longest]
        spots.append(tuple(where))
    return array.at[spots[0]].set(low).at[spots[1]].set(largest)


def spiked(values, own_key, source, target, shards_of, factor):
    def block_of(dim):
        return (jnp.arange(values.shape[dim]) // (values.shape[dim] // shards_of)).reshape((-1,) + (1,) * (values.ndim - 1 - dim))

    near = jax.random.permutation(own_key, shards_of)[block_of(target)]
    second = (block_of(target) + shards_of // 2) % shards_of
    return jnp.where((block_of(source) == near) | (block_of(source) == second), factor * values, values)


def level_of(rng, shape, cuts, smallest, top_value):
    gain, own = 1.0, jax.random.fold_in(rng, 6)
    for dim, shards_of in cuts:
        heights = jnp.exp(jax.random.uniform(jax.random.fold_in(own, dim), (shards_of,), jnp.float32, smallest / len(cuts), top_value / len(cuts)))
        gain = gain * jnp.repeat(heights, shape[dim] // shards_of).reshape([-1 if axis == dim else 1 for axis in range(len(shape))])
    return gain


def normal_values(stream_key, extent, scale, bound, cuts=(), held_as=jnp.bfloat16):
    drawn = scale * jax.random.normal(stream_key, extent, jnp.float32)
    if cuts:
        drawn = drawn * level_of(stream_key, extent, cuts, -0.22, 0.18)
    return jnp.clip(drawn, -bound, bound).astype(held_as)


def heavy_noise(key, extent, scale, reach, pieces, heavy, held_as=jnp.bfloat16):
    values = scale * jax.random.normal(key, extent, jnp.float32)
    if pieces:
        values = values * level_of(key, extent, pieces, -0.22, 0.18)
    return jnp.clip(spiked(values, jax.random.fold_in(key, 3), *heavy), -reach, reach).astype(held_as)


def setup_inputs(seed: int = 0) -> dict:
    splits = jax.random.split(jax.random.key(seed), 26)
    text_in = heavy_noise(splits[0], (PAIRS, LT, DT), 1.0, 6.0, ((0, 32),), (0, 2, 32, 2.75))
    image_in = heavy_noise(splits[1], (PAIRS, LV, DV), 1.0, 6.0, ((0, 32),), (0, 2, 32, 2.75))
    text_lengths = draw_text_lengths(jax.random.fold_in(splits[25], 71), 0)
    region_mask = set_ends((jax.random.randint(splits[3], (PAIRS, LV), 0, 4) < 3).astype(jnp.int32), jax.random.fold_in(splits[3], 1), 0, 1)
    text_cot = normal_values(splits[4], (PAIRS, LT, DT), 1.0, 6.0, ((0, 32),))
    image_cot = normal_values(splits[5], (PAIRS, LV, DV), 1.0, 6.0, ((0, 32),))
    co_text_proj = normal_values(splits[6], (3, DT, CO), DT ** -0.5, 0.21875, ((1, 32),))
    co_image_proj = normal_values(splits[7], (3, DV, CO), DV ** -0.5, 0.1875, ((1, 32),))
    co_bias = normal_values(splits[8], (4, CO), 0.5, 3.0, ((1, 32),))
    co_text_out = normal_values(splits[9], (CO, DT), (CO // 16) ** -0.5, 0.75, ((0, 32),))
    co_image_out = normal_values(splits[10], (CO, DV), (CO // 16) ** -0.5, 0.75, ((0, 32),))
    text_up = normal_values(splits[11], (DT, FT), DT ** -0.5, 0.21875, ((0, 32),))
    text_up_bias = normal_values(splits[12], (FT,), 0.5, 3.0, ((0, 32),))
    text_down = normal_values(splits[13], (FT, DT), FT ** -0.5, 0.109375, ((0, 32),))
    image_up = normal_values(splits[14], (DV, FV), DV ** -0.5, 0.1875, ((0, 32),))
    image_up_bias = normal_values(splits[15], (FV,), 0.5, 3.0, ((0, 32),))
    image_down = normal_values(splits[16], (FV, DV), FV ** -0.5, 0.1875, ((0, 32),))
    text_self_qkv = normal_values(splits[17], (3, DT, DT), DT ** -0.5, 0.21875, ((1, 32),))
    text_self_out = normal_values(splits[18], (DT, DT), (DT // 16) ** -0.5, 0.875, ((0, 32),))
    image_self_qkv = normal_values(splits[19], (3, DV, DV), DV ** -0.5, 0.1875, ((1, 32),))
    image_self_out = normal_values(splits[20], (DV, DV), (DV // 16) ** -0.5, 0.75, ((0, 32),))
    text_gains = jnp.clip(1.0 + 0.1 * jax.random.normal(splits[21], (3, DT), jnp.float32), 0.5, 1.5).astype(jnp.bfloat16)
    image_gains = jnp.clip(1.0 + 0.1 * jax.random.normal(splits[22], (3, DV), jnp.float32), 0.5, 1.5).astype(jnp.bfloat16)
    text_vectors = normal_values(splits[23], (8, DT), 0.5, 3.0, ((1, 32),))
    image_vectors = normal_values(splits[24], (8, DV), 0.5, 3.0, ((1, 32),))
    return dict(text_in=text_in, image_in=image_in, text_lengths=text_lengths, region_mask=region_mask, text_cot=text_cot, image_cot=image_cot, co_text_proj=co_text_proj, co_image_proj=co_image_proj, co_bias=co_bias, co_text_out=co_text_out, co_image_out=co_image_out, text_up=text_up, text_up_bias=text_up_bias, text_down=text_down, image_up=image_up, image_up_bias=image_up_bias, image_down=image_down, text_self_qkv=text_self_qkv, text_self_out=text_self_out, image_self_qkv=image_self_qkv, image_self_out=image_self_out, text_gains=text_gains, image_gains=image_gains, text_vectors=text_vectors, image_vectors=image_vectors)


EPSILON = 1e-06
MASKED = -30000.0
ROOT_HALF = 0.7071067811865476
HIGH = lax.Precision.HIGHEST

@jax.custom_vjp
def low(v):
    return lax.optimization_barrier(v.astype(jnp.bfloat16)).astype(jnp.float32)

@jax.custom_vjp
def low_back(v):
    return v

def low_keep(v):
    return (low(v), None)

def low_pass(kept, grad):
    return (grad,)

def back_keep(v):
    return (v, None)

def back_low(kept, grad):
    return (low(grad),)
low.defvjp(low_keep, low_pass)
low_back.defvjp(back_keep, back_low)

def low_both(values):
    return low(low_back(values))

def linear(inputs, weight):
    return jnp.einsum('...i,ij->...j', inputs, weight, precision=HIGH)

def layer_norm(values, scale_gain, offset):
    center = values - lax.optimization_barrier(jnp.mean(values, -1, keepdims=True))
    spread = lax.optimization_barrier(jnp.mean(center * center, -1, keepdims=True))
    return center * lax.rsqrt(spread + EPSILON) * scale_gain + offset

def gelu_exact(values):
    return 0.5 * values * (1.0 + lax.erf(values * ROOT_HALF))

def attend(queries, key_rows, values, key_live, head_count):
    group_size, query_len, feature_width = queries.shape
    key_len = key_rows.shape[1]
    head_size = feature_width // head_count
    query_heads = queries.reshape(group_size, query_len, head_count, head_size)
    key_heads = key_rows.reshape(group_size, key_len, head_count, head_size)
    value_heads = values.reshape(group_size, key_len, head_count, head_size)
    scores = low_back(jnp.einsum('gqhd,gkhd->ghqk', query_heads, key_heads, precision=HIGH) * head_size ** (-0.5))
    scores = scores + jnp.where(key_live[:, None, None, :], 0.0, MASKED)
    shifted = scores - lax.optimization_barrier(jnp.max(scores, -1, keepdims=True))
    exponent = jnp.exp(shifted)
    attention = exponent / lax.optimization_barrier(jnp.sum(exponent, -1, keepdims=True))
    mixture = jnp.einsum('ghqk,gkhd->gqhd', low(attention), value_heads, precision=HIGH)
    return low_both(mixture.reshape(group_size, query_len, feature_width))

def feed_forward(normed, up_weight, up_bias, down_weight, down_bias, scale_gain, offset):
    hidden = low(gelu_exact(low_back(linear(low(normed), up_weight) + up_bias)))
    return layer_norm(normed + low_back(linear(hidden, down_weight) + down_bias), scale_gain, offset)

def self_block(second, qkv_weight, out_weight, vectors, scale_gain, key_live, head_count):
    second_low = low(second)
    queries = low_both(linear(second_low, qkv_weight[0]) + vectors[2])
    key_rows = low_both(linear(second_low, qkv_weight[1]))
    values = low_both(linear(second_low, qkv_weight[2]) + vectors[3])
    attended = attend(queries, key_rows, values, key_live, head_count)
    return layer_norm(second + low_back(linear(attended, out_weight) + vectors[4]), scale_gain, vectors[7])

def group_forward(params, text_rows, image_rows, text_live, region_live):
    co_text_proj, co_image_proj, co_bias, co_text_out, co_image_out, text_up, text_up_bias, text_down, image_up, image_up_bias, image_down, text_self_qkv, text_self_out, image_self_qkv, image_self_out, text_gains, image_gains, text_vectors, image_vectors = params
    text_query = low_both(linear(text_rows, co_text_proj[0]) + co_bias[0])
    text_key = low_both(linear(text_rows, co_text_proj[1]))
    text_value = low_both(linear(text_rows, co_text_proj[2]) + co_bias[1])
    image_query = low_both(linear(image_rows, co_image_proj[0]) + co_bias[2])
    image_key = low_both(linear(image_rows, co_image_proj[1]))
    image_value = low_both(linear(image_rows, co_image_proj[2]) + co_bias[3])
    text_mixture = attend(text_query, image_key, image_value, region_live, CHN)
    image_mixture = attend(image_query, text_key, text_value, text_live, CHN)
    text_first = layer_norm(text_rows + low_back(linear(text_mixture, co_text_out) + text_vectors[0]), text_gains[0], text_vectors[5])
    image_first = layer_norm(image_rows + low_back(linear(image_mixture, co_image_out) + image_vectors[0]), image_gains[0], image_vectors[5])
    text_second = feed_forward(text_first, text_up, text_up_bias, text_down, text_vectors[1], text_gains[1], text_vectors[6])
    image_second = feed_forward(image_first, image_up, image_up_bias, image_down, image_vectors[1], image_gains[1], image_vectors[6])
    text_final = self_block(text_second, text_self_qkv, text_self_out, text_vectors, text_gains[2], text_live, HT)
    image_final = self_block(image_second, image_self_qkv, image_self_out, image_vectors, image_gains[2], region_live, HV)
    return (text_final, image_final)

def reference(text_in, image_in, text_lengths, region_mask, text_cot, image_cot, co_text_proj, co_image_proj, co_bias, co_text_out, co_image_out, text_up, text_up_bias, text_down, image_up, image_up_bias, image_down, text_self_qkv, text_self_out, image_self_qkv, image_self_out, text_gains, image_gains, text_vectors, image_vectors):
    params = tuple((weight.astype(jnp.float32) for weight in (co_text_proj, co_image_proj, co_bias, co_text_out, co_image_out, text_up, text_up_bias, text_down, image_up, image_up_bias, image_down, text_self_qkv, text_self_out, image_self_qkv, image_self_out, text_gains, image_gains, text_vectors, image_vectors)))
    text_live = jnp.arange(LT, dtype=jnp.int32)[None, :] < text_lengths[:, None]
    region_live = region_mask > 0
    group_size = math.gcd(PAIRS, 32)
    group_count = PAIRS // group_size

    def forward_all(weights, text_rows, image_rows):

        def forward_group(blocks):
            return group_forward(weights, blocks[0], blocks[1], blocks[2], blocks[3])
        results = lax.map(jax.checkpoint(forward_group), (text_rows.reshape(group_count, group_size, LT, DT), image_rows.reshape(group_count, group_size, LV, DV), text_live.reshape(group_count, group_size, LT), region_live.reshape(group_count, group_size, LV)))
        return (results[0].reshape(PAIRS, LT, DT), results[1].reshape(PAIRS, LV, DV))
    (text_final, image_final), pullback = jax.vjp(forward_all, params, text_in.astype(jnp.float32), image_in.astype(jnp.float32))
    param_grads, text_grad, image_grad = pullback((text_cot.astype(jnp.float32), image_cot.astype(jnp.float32)))
    return (text_final.astype(jnp.bfloat16), image_final.astype(jnp.bfloat16), text_grad.astype(jnp.bfloat16), image_grad.astype(jnp.bfloat16), param_grads[0], param_grads[1], param_grads[2], param_grads[3], param_grads[4], param_grads[5], param_grads[6], param_grads[7], param_grads[8], param_grads[9], param_grads[10], param_grads[11], param_grads[12], param_grads[13], param_grads[14], param_grads[15], param_grads[16], param_grads[17], param_grads[18])
```

```python
import functools

import jax
import jax.numpy as jnp
from jax import lax
from jax.experimental import pallas as pl
from jax.experimental.pallas import tpu as pltpu
from jax.sharding import PartitionSpec as P

MESH = pl.DeviceIdType.MESH
ORDERS = ((2, 0, 1), (2, 1, 0))

def place_of(sizes):
    X, Y, Z = sizes
    gx, gy = lax.axis_index("gx"), lax.axis_index("gy")
    return (gx // 2, gy % Y, gy // Y), gx % 2

def device_of(sizes, place, core):
    return (place[0] * 2 + core, place[2] * sizes[1] + place[1])

def shifted(sizes, place, dim, step):
    return tuple(lax.rem(p + step, sizes[dim]) if i == dim else p for i, p in enumerate(place))

def greet(sizes, place, core):
    barrier = pltpu.get_barrier_semaphore()
    count = 1
    pl.semaphore_signal(barrier, inc=1, device_id=device_of(sizes, place, 1 - core), device_id_type=MESH)
    for dim in range(3):
        for step in range(1, sizes[dim]):
            pl.semaphore_signal(barrier, inc=1, device_id=device_of(sizes, shifted(sizes, place, dim, step), core), device_id_type=MESH)
            count += 1
    pl.semaphore_wait(barrier, count)

def slot_base(sizes):
    return {0: 0, 1: sizes[0] - 1, 2: sizes[0] + sizes[1] - 2}

def gather_kernel(sizes, pieces, ahead, *refs):
    n_in = max(p[0] for p in pieces) + 1
    n = len(pieces)
    ins, outs = refs[:n_in], refs[n_in:n_in + n]
    send, recv, own = refs[n_in + n:]
    place, core = place_of(sizes)
    x, y, z = place
    base = slot_base(sizes)
    last = sum(sizes) - 3
    greet(sizes, place, core)
    def src_of(m):
        number, index, _ = pieces[m]
        return ins[number] if index is None else ins[number].at[index]
    keep = []
    for m in range(n):
        copy = pltpu.make_async_copy(src_of(m), outs[m].at[x, core, z, y], own.at[m])
        copy.start()
        keep.append(copy)
    def view(m, where, opened):
        px, py, pz = (slice(None) if d in opened else where[d] for d in range(3))
        return outs[m].at[px, core, pz, py]
    started = []
    arrive = {}
    def start(m, phase):
        order = ORDERS[pieces[m][2]]
        waits = []
        if phase == 3:
            part = outs[m].at[:, core]
            copy = pltpu.make_async_remote_copy(part, part, send.at[m, last], recv.at[m, last],
                device_id=device_of(sizes, place, 1 - core), device_id_type=MESH)
            copy.start()
            started.append(copy)
            waits.append(pltpu.make_async_remote_copy(outs[m].at[:, 1 - core], outs[m].at[:, 1 - core], send.at[m, last], recv.at[m, last],
                device_id=device_of(sizes, place, 1 - core), device_id_type=MESH))
        else:
            dim = order[phase]
            opened = order[:phase]
            part = view(m, place, opened)
            source = src_of(m) if phase == 0 else part
            for step in range(1, sizes[dim]):
                slot = base[dim] + step - 1
                peer = shifted(sizes, place, dim, step)
                back = shifted(sizes, place, dim, sizes[dim] - step)
                copy = pltpu.make_async_remote_copy(source, part, send.at[m, slot], recv.at[m, slot],
                    device_id=device_of(sizes, peer, core), device_id_type=MESH)
                copy.start()
                started.append(copy)
                came = view(m, back, opened)
                waits.append(pltpu.make_async_remote_copy(came, came, send.at[m, slot], recv.at[m, slot],
                    device_id=device_of(sizes, peer, core), device_id_type=MESH))
        arrive[m, phase] = waits
    def settle(m, phase):
        for w in arrive[m, phase]:
            w.wait_recv()
    for s in range(n + 3 + ahead):
        if s < n:
            start(s, 0)
        for phase in (1, 2, 3):
            m = s - ahead - phase + 1
            if 0 <= m < n:
                settle(m, phase - 1)
                if phase == 1:
                    keep[m].wait()
                start(m, phase)
    for m in range(n):
        settle(m, 3)
    for c in started:
        c.wait_send()

def gather(sizes, inputs, pieces, ahead=3, collective_id=0):
    X, Y, Z = sizes
    outs = []
    for number, index, _ in pieces:
        a = inputs[number]
        outs.append(jax.ShapeDtypeStruct((X, 2, Z, Y) + a.shape[(0 if index is None else 1):], a.dtype))
    n = len(pieces)
    slots = sum(sizes) - 2
    return pl.pallas_call(
        functools.partial(gather_kernel, sizes, pieces, ahead),
        out_shape=outs,
        in_specs=[pl.BlockSpec(memory_space=pl.ANY)] * len(inputs),
        out_specs=[pl.BlockSpec(memory_space=pl.ANY)] * n,
        scratch_shapes=[pltpu.SemaphoreType.DMA((n, slots)), pltpu.SemaphoreType.DMA((n, slots)), pltpu.SemaphoreType.DMA((n,))],
        compiler_params=pltpu.CompilerParams(collective_id=collective_id, has_side_effects=True),
    )(*inputs)

def mesh_sizes(mesh):
    ys = len({d.coords[1] for d in mesh.devices.flat})
    return (mesh.shape["gx"] // 2, ys, mesh.shape["gy"] // ys)


def pack_small(small):
    flat = jnp.concatenate([a.reshape(-1) for a in small])
    return jnp.pad(flat, (0, 1024 - flat.shape[0])).reshape(8, 128)


def unpack_small(full, small):
    count = full.shape[0] // 8
    rows = full.reshape(count, 1024)
    outs, at = [], 0
    for a in small:
        part = rows[:, at:at + a.size]
        at += a.size
        if a.ndim == 1:
            outs.append(part.reshape(-1))
        else:
            part = part.reshape(count, *a.shape).transpose(1, 0, 2)
            outs.append(part.reshape(a.shape[0], -1))
    return outs


def gather_all(sizes, packed, big):
    inputs = (packed, *big)
    pieces = [(0, None, 0)]
    for number, a in enumerate(big):
        for index in range(3) if a.ndim == 3 else (None,):
            pieces.append((number + 1, index, len(pieces) % 2))
    outs = gather(sizes, inputs, pieces)
    return [o.reshape(-1, o.shape[-1]) for o in outs]


HT = 12
HV = 8
CHN = 8


EPSILON = 1e-06
MASKED = -30000.0
ROOT_HALF = 0.7071067811865476


def layer_norm(values, scale_gain, offset):
    center = values - jnp.mean(values, -1, keepdims=True)
    spread = jnp.mean(center * center, -1, keepdims=True)
    return center * lax.rsqrt(spread + EPSILON) * scale_gain + offset


def gelu_exact(values):
    return 0.5 * values * (1.0 + lax.erf(values * ROOT_HALF))


def project(inputs, weight):
    return jnp.dot(inputs, weight, preferred_element_type=jnp.float32)


def linear_back(inputs, weight, grad_low):
    weight_grad = lax.dot_general(
        inputs, grad_low, (((0,), (0,)), ((), ())), preferred_element_type=jnp.float32
    )
    input_grad = lax.dot_general(
        grad_low, weight, (((1,), (1,)), ((), ())), preferred_element_type=jnp.float32
    )
    bias_grad = jnp.sum(grad_low.astype(jnp.float32), 0)
    return (weight_grad, bias_grad, input_grad)


def split_heads(values, pair_count, head_count):
    row_count, feature_width = values.shape
    return values.reshape(
        pair_count, row_count // pair_count, head_count, feature_width // head_count
    )


def attention_scores(queries, key_rows, key_live, head_count, pair_count):
    query_heads = split_heads(queries, pair_count, head_count)
    key_heads = split_heads(key_rows, pair_count, head_count)
    score_scale = (queries.shape[1] // head_count) ** (-0.5)
    scores = (
        jnp.einsum("pqhd,pkhd->phqk", query_heads, key_heads, preferred_element_type=jnp.float32)
        * score_scale
    )
    return scores + jnp.where(key_live[:, None, None, :], 0.0, MASKED)


def attend_forward(queries, key_rows, values, key_live, head_count, pair_count):
    scores = attention_scores(queries, key_rows, key_live, head_count, pair_count)
    row_max = jnp.max(scores, -1, keepdims=True)
    log_total = row_max + jnp.log(jnp.sum(jnp.exp(scores - row_max), -1, keepdims=True))
    attention = jnp.exp(scores - log_total).astype(jnp.bfloat16)
    value_heads = split_heads(values, pair_count, head_count)
    mixture = jnp.einsum(
        "phqk,pkhd->pqhd", attention, value_heads, preferred_element_type=jnp.float32
    )
    return (mixture.reshape(queries.shape[0], values.shape[1]).astype(jnp.bfloat16), log_total)


def attend_backward(
    queries, key_rows, values, key_live, head_count, pair_count, log_total, grad_low
):
    scores = attention_scores(queries, key_rows, key_live, head_count, pair_count)
    attention = jnp.exp(scores - log_total)
    attention_low = attention.astype(jnp.bfloat16)
    query_heads = split_heads(queries, pair_count, head_count)
    key_heads = split_heads(key_rows, pair_count, head_count)
    value_heads = split_heads(values, pair_count, head_count)
    grad_heads = split_heads(grad_low, pair_count, head_count)
    value_grad = jnp.einsum(
        "phqk,pqhd->pkhd", attention_low, grad_heads, preferred_element_type=jnp.float32
    )
    attention_grad = jnp.einsum(
        "pqhd,pkhd->phqk", grad_heads, value_heads, preferred_element_type=jnp.float32
    )
    score_grad = (
        attention * (attention_grad - jnp.sum(attention * attention_grad, -1, keepdims=True))
    ).astype(jnp.bfloat16)
    score_scale = (queries.shape[1] // head_count) ** (-0.5)
    query_grad = (
        jnp.einsum("phqk,pkhd->pqhd", score_grad, key_heads, preferred_element_type=jnp.float32)
        * score_scale
    )
    key_grad = (
        jnp.einsum("phqk,pqhd->pkhd", score_grad, query_heads, preferred_element_type=jnp.float32)
        * score_scale
    )
    return (
        query_grad.reshape(queries.shape).astype(jnp.bfloat16),
        key_grad.reshape(key_rows.shape).astype(jnp.bfloat16),
        value_grad.reshape(values.shape).astype(jnp.bfloat16),
    )


def projections_back(inputs, weights, grads):
    outcomes = [linear_back(inputs, weights[position], grads[position]) for position in range(3)]
    stacked = jnp.stack([outcome[0] for outcome in outcomes])
    input_grad = outcomes[0][2] + outcomes[1][2] + outcomes[2][2]
    return (stacked, outcomes[0][1], outcomes[2][1], input_grad)


def feed_forward(normed, up_weight, up_bias, down_weight, down_bias, scale_gain, offset):
    normed_low = normed.astype(jnp.bfloat16)
    pre_act = project(normed_low, up_weight) + up_bias
    hidden, gelu_back = jax.vjp(gelu_exact, pre_act)
    hidden_low = hidden.astype(jnp.bfloat16)
    branch = project(hidden_low, down_weight) + down_bias
    second, norm_back = jax.vjp(layer_norm, normed + branch, scale_gain, offset)
    return (second, (normed_low, hidden_low, gelu_back, norm_back))


def feed_back(kept, up_weight, down_weight, grad_second):
    normed_low, hidden_low, gelu_back, norm_back = kept
    pre_grad, gain_grad, shift_grad = norm_back(grad_second)
    down_grad, down_bias_grad, hidden_grad = linear_back(
        hidden_low, down_weight, pre_grad.astype(jnp.bfloat16)
    )
    (act_grad,) = gelu_back(hidden_grad)
    up_grad, up_bias_grad, normed_grad = linear_back(
        normed_low, up_weight, act_grad.astype(jnp.bfloat16)
    )
    return (
        up_grad,
        up_bias_grad,
        down_grad,
        down_bias_grad,
        gain_grad,
        shift_grad,
        pre_grad + normed_grad,
    )


def self_block(
    second, qkv_weight, out_weight, vectors, scale_gain, key_live, head_count, pair_count
):
    second_low = second.astype(jnp.bfloat16)
    queries = (project(second_low, qkv_weight[0]) + vectors[2]).astype(jnp.bfloat16)
    key_rows = project(second_low, qkv_weight[1]).astype(jnp.bfloat16)
    values = (project(second_low, qkv_weight[2]) + vectors[3]).astype(jnp.bfloat16)
    mixture, log_total = attend_forward(queries, key_rows, values, key_live, head_count, pair_count)
    final, norm_back = jax.vjp(
        layer_norm, second + project(mixture, out_weight) + vectors[4], scale_gain, vectors[7]
    )
    return (final, (second_low, queries, key_rows, values, mixture, log_total, norm_back))


def self_back(kept, qkv_weight, out_weight, key_live, head_count, pair_count, grad_final):
    second_low, queries, key_rows, values, mixture, log_total, norm_back = kept
    pre_grad, gain_grad, shift_grad = norm_back(grad_final)
    out_grad, out_bias_grad, mixture_grad = linear_back(
        mixture, out_weight, pre_grad.astype(jnp.bfloat16)
    )
    query_grad, key_grad, value_grad = attend_backward(
        queries,
        key_rows,
        values,
        key_live,
        head_count,
        pair_count,
        log_total,
        mixture_grad.astype(jnp.bfloat16),
    )
    qkv_grad, query_bias_grad, value_bias_grad, input_grad = projections_back(
        second_low, qkv_weight, (query_grad, key_grad, value_grad)
    )
    return (
        qkv_grad,
        out_grad,
        query_bias_grad,
        value_bias_grad,
        out_bias_grad,
        gain_grad,
        shift_grad,
        pre_grad + input_grad,
    )


def per_device(
    sizes,
    text_in,
    image_in,
    text_lengths,
    region_mask,
    text_cot,
    image_cot,
    co_text_proj,
    co_image_proj,
    co_bias,
    co_text_out,
    co_image_out,
    text_up,
    text_up_bias,
    text_down,
    image_up,
    image_up_bias,
    image_down,
    text_self_qkv,
    text_self_out,
    image_self_qkv,
    image_self_out,
    text_gains,
    image_gains,
    text_vectors,
    image_vectors,
):
    pair_count, text_len, text_width = text_in.shape
    region_count = image_in.shape[1]
    image_width = image_in.shape[2]
    text_rows = text_in.reshape(pair_count * text_len, text_width)
    image_rows = image_in.reshape(pair_count * region_count, image_width)
    text_live = lax.broadcasted_iota(jnp.int32, (pair_count, text_len), 1) < text_lengths[:, None]
    region_live = region_mask > 0
    small = (co_bias, text_gains, image_gains, text_vectors, image_vectors, text_up_bias, image_up_bias)
    big = (
        co_text_proj, co_image_proj, co_text_out, co_image_out, text_up, text_down, image_up, image_down,
        text_self_qkv, text_self_out, image_self_qkv, image_self_out,
    )
    full = gather_all(sizes, pack_small(small), big)
    (
        cross_bias_all, text_gain_all, image_gain_all, text_vector_all, image_vector_all,
        text_up_bias_all, image_up_bias_all,
    ) = unpack_small(full[0], small)
    text_proj_all, image_proj_all = full[1:4], full[4:7]
    text_out_all, image_out_all = full[7], full[8]
    feed_full = (full[9], text_up_bias_all, full[10], full[11], image_up_bias_all, full[12])
    self_full = (full[13:16], full[16], full[17:20], full[20])
    cross_bias_float = cross_bias_all.astype(jnp.float32)
    text_gain_float = text_gain_all.astype(jnp.float32)
    image_gain_float = image_gain_all.astype(jnp.float32)
    text_vector_float = text_vector_all.astype(jnp.float32)
    image_vector_float = image_vector_all.astype(jnp.float32)
    text_query = (project(text_rows, text_proj_all[0]) + cross_bias_float[0]).astype(jnp.bfloat16)
    text_key = project(text_rows, text_proj_all[1]).astype(jnp.bfloat16)
    text_value = (project(text_rows, text_proj_all[2]) + cross_bias_float[1]).astype(jnp.bfloat16)
    image_query = (project(image_rows, image_proj_all[0]) + cross_bias_float[2]).astype(
        jnp.bfloat16
    )
    image_key = project(image_rows, image_proj_all[1]).astype(jnp.bfloat16)
    image_value = (project(image_rows, image_proj_all[2]) + cross_bias_float[3]).astype(
        jnp.bfloat16
    )
    text_mixture, text_log = attend_forward(
        text_query, image_key, image_value, region_live, CHN, pair_count
    )
    image_mixture, image_log = attend_forward(
        image_query, text_key, text_value, text_live, CHN, pair_count
    )
    text_normed, text_norm_back = jax.vjp(
        layer_norm,
        text_rows.astype(jnp.float32) + project(text_mixture, text_out_all) + text_vector_float[0],
        text_gain_float[0],
        text_vector_float[5],
    )
    image_normed, image_norm_back = jax.vjp(
        layer_norm,
        image_rows.astype(jnp.float32)
        + project(image_mixture, image_out_all)
        + image_vector_float[0],
        image_gain_float[0],
        image_vector_float[5],
    )
    text_second, text_feed_kept = feed_forward(
        text_normed,
        feed_full[0],
        feed_full[1].astype(jnp.float32),
        feed_full[2],
        text_vector_float[1],
        text_gain_float[1],
        text_vector_float[6],
    )
    image_second, image_feed_kept = feed_forward(
        image_normed,
        feed_full[3],
        feed_full[4].astype(jnp.float32),
        feed_full[5],
        image_vector_float[1],
        image_gain_float[1],
        image_vector_float[6],
    )
    text_final, text_self_kept = self_block(
        text_second,
        self_full[0],
        self_full[1],
        text_vector_float,
        text_gain_float[2],
        text_live,
        HT,
        pair_count,
    )
    image_final, image_self_kept = self_block(
        image_second,
        self_full[2],
        self_full[3],
        image_vector_float,
        image_gain_float[2],
        region_live,
        HV,
        pair_count,
    )
    text_out = text_final.astype(jnp.bfloat16).reshape(pair_count, text_len, text_width)
    image_out = image_final.astype(jnp.bfloat16).reshape(pair_count, region_count, image_width)
    text_self_grads = self_back(
        text_self_kept,
        self_full[0],
        self_full[1],
        text_live,
        HT,
        pair_count,
        text_cot.reshape(pair_count * text_len, text_width).astype(jnp.float32),
    )
    image_self_grads = self_back(
        image_self_kept,
        self_full[2],
        self_full[3],
        region_live,
        HV,
        pair_count,
        image_cot.reshape(pair_count * region_count, image_width).astype(jnp.float32),
    )
    self_partial = (
        lax.psum_scatter(
            text_self_grads[0].astype(jnp.bfloat16), "gx", scatter_dimension=1, tiled=True
        ).astype(jnp.float32),
        lax.psum_scatter(
            text_self_grads[1].astype(jnp.bfloat16), "gx", scatter_dimension=0, tiled=True
        ).astype(jnp.float32),
        lax.psum_scatter(
            image_self_grads[0].astype(jnp.bfloat16), "gx", scatter_dimension=1, tiled=True
        ).astype(jnp.float32),
        lax.psum_scatter(
            image_self_grads[1].astype(jnp.bfloat16), "gx", scatter_dimension=0, tiled=True
        ).astype(jnp.float32),
    )
    self_sums = (
        lax.psum_scatter(
            self_partial[0].astype(jnp.bfloat16), "gy", scatter_dimension=1, tiled=True
        ).astype(jnp.float32),
        lax.psum_scatter(
            self_partial[1].astype(jnp.bfloat16), "gy", scatter_dimension=0, tiled=True
        ).astype(jnp.float32),
        lax.psum_scatter(
            self_partial[2].astype(jnp.bfloat16), "gy", scatter_dimension=1, tiled=True
        ).astype(jnp.float32),
        lax.psum_scatter(
            self_partial[3].astype(jnp.bfloat16), "gy", scatter_dimension=0, tiled=True
        ).astype(jnp.float32),
    )
    text_feed_grads = feed_back(
        text_feed_kept, feed_full[0], feed_full[2], text_self_grads[7]
    )
    image_feed_grads = feed_back(
        image_feed_kept, feed_full[3], feed_full[5], image_self_grads[7]
    )
    feed_partial = (
        lax.psum_scatter(
            text_feed_grads[0].astype(jnp.bfloat16), "gx", scatter_dimension=0, tiled=True
        ).astype(jnp.float32),
        lax.psum_scatter(
            text_feed_grads[1].astype(jnp.bfloat16), "gx", scatter_dimension=0, tiled=True
        ).astype(jnp.float32),
        lax.psum_scatter(
            text_feed_grads[2].astype(jnp.bfloat16), "gx", scatter_dimension=0, tiled=True
        ).astype(jnp.float32),
        lax.psum_scatter(
            image_feed_grads[0].astype(jnp.bfloat16), "gx", scatter_dimension=0, tiled=True
        ).astype(jnp.float32),
        lax.psum_scatter(
            image_feed_grads[1].astype(jnp.bfloat16), "gx", scatter_dimension=0, tiled=True
        ).astype(jnp.float32),
        lax.psum_scatter(
            image_feed_grads[2].astype(jnp.bfloat16), "gx", scatter_dimension=0, tiled=True
        ).astype(jnp.float32),
    )
    feed_sums = (
        lax.psum_scatter(
            feed_partial[0].astype(jnp.bfloat16), "gy", scatter_dimension=0, tiled=True
        ).astype(jnp.float32),
        lax.psum_scatter(
            feed_partial[1].astype(jnp.bfloat16), "gy", scatter_dimension=0, tiled=True
        ).astype(jnp.float32),
        lax.psum_scatter(
            feed_partial[2].astype(jnp.bfloat16), "gy", scatter_dimension=0, tiled=True
        ).astype(jnp.float32),
        lax.psum_scatter(
            feed_partial[3].astype(jnp.bfloat16), "gy", scatter_dimension=0, tiled=True
        ).astype(jnp.float32),
        lax.psum_scatter(
            feed_partial[4].astype(jnp.bfloat16), "gy", scatter_dimension=0, tiled=True
        ).astype(jnp.float32),
        lax.psum_scatter(
            feed_partial[5].astype(jnp.bfloat16), "gy", scatter_dimension=0, tiled=True
        ).astype(jnp.float32),
    )
    text_pre_grad, text_first_gain_grad, text_first_shift_grad = text_norm_back(text_feed_grads[6])
    image_pre_grad, image_first_gain_grad, image_first_shift_grad = image_norm_back(
        image_feed_grads[6]
    )
    text_out_grad, text_out_bias_grad, text_mixture_grad = linear_back(
        text_mixture, text_out_all, text_pre_grad.astype(jnp.bfloat16)
    )
    image_out_grad, image_out_bias_grad, image_mixture_grad = linear_back(
        image_mixture, image_out_all, image_pre_grad.astype(jnp.bfloat16)
    )
    text_query_grad, image_key_grad, image_value_grad = attend_backward(
        text_query,
        image_key,
        image_value,
        region_live,
        CHN,
        pair_count,
        text_log,
        text_mixture_grad.astype(jnp.bfloat16),
    )
    image_query_grad, text_key_grad, text_value_grad = attend_backward(
        image_query,
        text_key,
        text_value,
        text_live,
        CHN,
        pair_count,
        image_log,
        image_mixture_grad.astype(jnp.bfloat16),
    )
    text_proj_grad, text_query_bias_grad, text_value_bias_grad, text_input_grad = projections_back(
        text_rows, text_proj_all, (text_query_grad, text_key_grad, text_value_grad)
    )
    image_proj_grad, image_query_bias_grad, image_value_bias_grad, image_input_grad = (
        projections_back(
            image_rows, image_proj_all, (image_query_grad, image_key_grad, image_value_grad)
        )
    )
    cross_bias_grad = jnp.stack(
        [text_query_bias_grad, text_value_bias_grad, image_query_bias_grad, image_value_bias_grad]
    )
    text_gains_grad = jnp.stack([text_first_gain_grad, text_feed_grads[4], text_self_grads[5]])
    image_gains_grad = jnp.stack([image_first_gain_grad, image_feed_grads[4], image_self_grads[5]])
    text_vectors_grad = jnp.stack(
        [
            text_out_bias_grad,
            text_feed_grads[3],
            text_self_grads[2],
            text_self_grads[3],
            text_self_grads[4],
            text_first_shift_grad,
            text_feed_grads[5],
            text_self_grads[6],
        ]
    )
    image_vectors_grad = jnp.stack(
        [
            image_out_bias_grad,
            image_feed_grads[3],
            image_self_grads[2],
            image_self_grads[3],
            image_self_grads[4],
            image_first_shift_grad,
            image_feed_grads[5],
            image_self_grads[6],
        ]
    )
    cross_partial = (
        lax.psum_scatter(
            text_proj_grad.astype(jnp.bfloat16), "gx", scatter_dimension=1, tiled=True
        ).astype(jnp.float32),
        lax.psum_scatter(
            image_proj_grad.astype(jnp.bfloat16), "gx", scatter_dimension=1, tiled=True
        ).astype(jnp.float32),
        lax.psum_scatter(
            cross_bias_grad.astype(jnp.bfloat16), "gx", scatter_dimension=1, tiled=True
        ).astype(jnp.float32),
        lax.psum_scatter(
            text_out_grad.astype(jnp.bfloat16), "gx", scatter_dimension=0, tiled=True
        ).astype(jnp.float32),
        lax.psum_scatter(
            image_out_grad.astype(jnp.bfloat16), "gx", scatter_dimension=0, tiled=True
        ).astype(jnp.float32),
        lax.psum_scatter(
            text_gains_grad.astype(jnp.bfloat16), "gx", scatter_dimension=1, tiled=True
        ).astype(jnp.float32),
        lax.psum_scatter(
            image_gains_grad.astype(jnp.bfloat16), "gx", scatter_dimension=1, tiled=True
        ).astype(jnp.float32),
        lax.psum_scatter(
            text_vectors_grad.astype(jnp.bfloat16), "gx", scatter_dimension=1, tiled=True
        ).astype(jnp.float32),
        lax.psum_scatter(
            image_vectors_grad.astype(jnp.bfloat16), "gx", scatter_dimension=1, tiled=True
        ).astype(jnp.float32),
    )
    cross_sums = (
        lax.psum_scatter(
            cross_partial[0].astype(jnp.bfloat16), "gy", scatter_dimension=1, tiled=True
        ).astype(jnp.float32),
        lax.psum_scatter(
            cross_partial[1].astype(jnp.bfloat16), "gy", scatter_dimension=1, tiled=True
        ).astype(jnp.float32),
        lax.psum_scatter(
            cross_partial[2].astype(jnp.bfloat16), "gy", scatter_dimension=1, tiled=True
        ).astype(jnp.float32),
        lax.psum_scatter(
            cross_partial[3].astype(jnp.bfloat16), "gy", scatter_dimension=0, tiled=True
        ).astype(jnp.float32),
        lax.psum_scatter(
            cross_partial[4].astype(jnp.bfloat16), "gy", scatter_dimension=0, tiled=True
        ).astype(jnp.float32),
        lax.psum_scatter(
            cross_partial[5].astype(jnp.bfloat16), "gy", scatter_dimension=1, tiled=True
        ).astype(jnp.float32),
        lax.psum_scatter(
            cross_partial[6].astype(jnp.bfloat16), "gy", scatter_dimension=1, tiled=True
        ).astype(jnp.float32),
        lax.psum_scatter(
            cross_partial[7].astype(jnp.bfloat16), "gy", scatter_dimension=1, tiled=True
        ).astype(jnp.float32),
        lax.psum_scatter(
            cross_partial[8].astype(jnp.bfloat16), "gy", scatter_dimension=1, tiled=True
        ).astype(jnp.float32),
    )
    text_in_grad = (
        (text_pre_grad + text_input_grad)
        .astype(jnp.bfloat16)
        .reshape(pair_count, text_len, text_width)
    )
    image_in_grad = (
        (image_pre_grad + image_input_grad)
        .astype(jnp.bfloat16)
        .reshape(pair_count, region_count, image_width)
    )
    return (
        text_out,
        image_out,
        text_in_grad,
        image_in_grad,
        cross_sums[0],
        cross_sums[1],
        cross_sums[2],
        cross_sums[3],
        cross_sums[4],
        feed_sums[0],
        feed_sums[1],
        feed_sums[2],
        feed_sums[3],
        feed_sums[4],
        feed_sums[5],
        self_sums[0],
        self_sums[1],
        self_sums[2],
        self_sums[3],
        cross_sums[5],
        cross_sums[6],
        cross_sums[7],
        cross_sums[8],
    )


def solution(mesh):
    placed = (
        P(("gx", "gy"), None, None),
        P(("gx", "gy"), None, None),
        P(("gx", "gy")),
        P(("gx", "gy"), None),
        P(("gx", "gy"), None, None),
        P(("gx", "gy"), None, None),
        P(None, ("gx", "gy"), None),
        P(None, ("gx", "gy"), None),
        P(None, ("gx", "gy")),
        P(("gx", "gy"), None),
        P(("gx", "gy"), None),
        P(("gx", "gy"), None),
        P(("gx", "gy")),
        P(("gx", "gy"), None),
        P(("gx", "gy"), None),
        P(("gx", "gy")),
        P(("gx", "gy"), None),
        P(None, ("gx", "gy"), None),
        P(("gx", "gy"), None),
        P(None, ("gx", "gy"), None),
        P(("gx", "gy"), None),
        P(None, ("gx", "gy")),
        P(None, ("gx", "gy")),
        P(None, ("gx", "gy")),
        P(None, ("gx", "gy")),
    )
    return jax.shard_map(
        functools.partial(per_device, mesh_sizes(mesh)),
        mesh=mesh,
        in_specs=placed,
        out_specs=(
            P(("gx", "gy"), None, None),
            P(("gx", "gy"), None, None),
            P(("gx", "gy"), None, None),
            P(("gx", "gy"), None, None),
            P(None, ("gx", "gy"), None),
            P(None, ("gx", "gy"), None),
            P(None, ("gx", "gy")),
            P(("gx", "gy"), None),
            P(("gx", "gy"), None),
            P(("gx", "gy"), None),
            P(("gx", "gy")),
            P(("gx", "gy"), None),
            P(("gx", "gy"), None),
            P(("gx", "gy")),
            P(("gx", "gy"), None),
            P(None, ("gx", "gy"), None),
            P(("gx", "gy"), None),
            P(None, ("gx", "gy"), None),
            P(("gx", "gy"), None),
            P(None, ("gx", "gy")),
            P(None, ("gx", "gy")),
            P(None, ("gx", "gy")),
            P(None, ("gx", "gy")),
        ),
        check_vma=False,
    )
```

```python
import functools

import jax
import jax.numpy as jnp
from jax import lax
from jax.experimental import pallas as pl
from jax.experimental.pallas import tpu as pltpu
from jax.sharding import PartitionSpec as P

MESH = pl.DeviceIdType.MESH
ORDERS = ((2, 0, 1), (2, 1, 0))

def place_of(sizes):
    X, Y, Z = sizes
    gx, gy = lax.axis_index("gx"), lax.axis_index("gy")
    return (gx // 2, gy % Y, gy // Y), gx % 2

def device_of(sizes, place, core):
    return (place[0] * 2 + core, place[2] * sizes[1] + place[1])

def shifted(sizes, place, dim, step):
    return tuple(lax.rem(p + step, sizes[dim]) if i == dim else p for i, p in enumerate(place))

def greet(sizes, place, core):
    barrier = pltpu.get_barrier_semaphore()
    count = 1
    pl.semaphore_signal(barrier, inc=1, device_id=device_of(sizes, place, 1 - core), device_id_type=MESH)
    for dim in range(3):
        for step in range(1, sizes[dim]):
            pl.semaphore_signal(barrier, inc=1, device_id=device_of(sizes, shifted(sizes, place, dim, step), core), device_id_type=MESH)
            count += 1
    pl.semaphore_wait(barrier, count)

def slot_base(sizes):
    return {0: 0, 1: sizes[0] - 1, 2: sizes[0] + sizes[1] - 2}

def gather_kernel(sizes, pieces, ahead, *refs):
    n_in = max(p[0] for p in pieces) + 1
    n = len(pieces)
    ins, outs = refs[:n_in], refs[n_in:n_in + n]
    send, recv, own = refs[n_in + n:]
    place, core = place_of(sizes)
    x, y, z = place
    base = slot_base(sizes)
    last = sum(sizes) - 3
    greet(sizes, place, core)
    def src_of(m):
        number, index, _ = pieces[m]
        return ins[number] if index is None else ins[number].at[index]
    keep = []
    for m in range(n):
        copy = pltpu.make_async_copy(src_of(m), outs[m].at[x, core, z, y], own.at[m])
        copy.start()
        keep.append(copy)
    def view(m, where, opened):
        px, py, pz = (slice(None) if d in opened else where[d] for d in range(3))
        return outs[m].at[px, core, pz, py]
    started = []
    arrive = {}
    def start(m, phase):
        order = ORDERS[pieces[m][2]]
        waits = []
        if phase == 3:
            part = outs[m].at[:, core]
            copy = pltpu.make_async_remote_copy(part, part, send.at[m, last], recv.at[m, last],
                device_id=device_of(sizes, place, 1 - core), device_id_type=MESH)
            copy.start()
            started.append(copy)
            waits.append(pltpu.make_async_remote_copy(outs[m].at[:, 1 - core], outs[m].at[:, 1 - core], send.at[m, last], recv.at[m, last],
                device_id=device_of(sizes, place, 1 - core), device_id_type=MESH))
        else:
            dim = order[phase]
            opened = order[:phase]
            part = view(m, place, opened)
            source = src_of(m) if phase == 0 else part
            for step in range(1, sizes[dim]):
                slot = base[dim] + step - 1
                peer = shifted(sizes, place, dim, step)
                back = shifted(sizes, place, dim, sizes[dim] - step)
                copy = pltpu.make_async_remote_copy(source, part, send.at[m, slot], recv.at[m, slot],
                    device_id=device_of(sizes, peer, core), device_id_type=MESH)
                copy.start()
                started.append(copy)
                came = view(m, back, opened)
                waits.append(pltpu.make_async_remote_copy(came, came, send.at[m, slot], recv.at[m, slot],
                    device_id=device_of(sizes, peer, core), device_id_type=MESH))
        arrive[m, phase] = waits
    def settle(m, phase):
        for w in arrive[m, phase]:
            w.wait_recv()
    for s in range(n + 3 + ahead):
        if s < n:
            start(s, 0)
        for phase in (1, 2, 3):
            m = s - ahead - phase + 1
            if 0 <= m < n:
                settle(m, phase - 1)
                if phase == 1:
                    keep[m].wait()
                start(m, phase)
    for m in range(n):
        settle(m, 3)
    for c in started:
        c.wait_send()

def gather(sizes, inputs, pieces, ahead=3, collective_id=0):
    X, Y, Z = sizes
    outs = []
    for number, index, _ in pieces:
        a = inputs[number]
        outs.append(jax.ShapeDtypeStruct((X, 2, Z, Y) + a.shape[(0 if index is None else 1):], a.dtype))
    n = len(pieces)
    slots = sum(sizes) - 2
    return pl.pallas_call(
        functools.partial(gather_kernel, sizes, pieces, ahead),
        out_shape=outs,
        in_specs=[pl.BlockSpec(memory_space=pl.ANY)] * len(inputs),
        out_specs=[pl.BlockSpec(memory_space=pl.ANY)] * n,
        scratch_shapes=[pltpu.SemaphoreType.DMA((n, slots)), pltpu.SemaphoreType.DMA((n, slots)), pltpu.SemaphoreType.DMA((n,))],
        compiler_params=pltpu.CompilerParams(collective_id=collective_id, has_side_effects=True),
    )(*inputs)

def mesh_sizes(mesh):
    ys = len({d.coords[1] for d in mesh.devices.flat})
    return (mesh.shape["gx"] // 2, ys, mesh.shape["gy"] // ys)


def pack_small(small):
    flat = jnp.concatenate([a.reshape(-1) for a in small])
    return jnp.pad(flat, (0, 1024 - flat.shape[0])).reshape(8, 128)


def unpack_small(full, small):
    count = full.shape[0] // 8
    rows = full.reshape(count, 1024)
    outs, at = [], 0
    for a in small:
        part = rows[:, at:at + a.size]
        at += a.size
        if a.ndim == 1:
            outs.append(part.reshape(-1))
        else:
            part = part.reshape(count, *a.shape).transpose(1, 0, 2)
            outs.append(part.reshape(a.shape[0], -1))
    return outs


def gather_all(sizes, packed, big):
    inputs = (packed, *big)
    pieces = [(0, None, 0)]
    for number, a in enumerate(big):
        for index in range(3) if a.ndim == 3 else (None,):
            pieces.append((number + 1, index, len(pieces) % 2))
    outs = gather(sizes, inputs, pieces)
    return [o.reshape(-1, o.shape[-1]) for o in outs]


FIRST = ((1, 0, 2), (0, 1, 2))
TILE = 256


def block_axis(dim):
    return (0, 3, 2)[dim]


def arrange(sizes, order, values, rows):
    X, Y, Z = sizes
    count, width = values.shape
    depth = width // (2 * X * Y * Z)
    a = jnp.pad(values, ((0, rows - count), (0, 0))).T.reshape(X, 2, Z, Y, depth, rows)
    first, second, third = (block_axis(d) for d in order)
    a = a.transpose(1, first, second, third, 4, 5)
    return a.reshape(2, sizes[order[0]], sizes[order[1]], sizes[order[2]] * depth, rows)


def scatter_kernel(sizes, jobs, n_act, *refs):
    n_grad = len(jobs)
    n_out = max(j[2] for j in jobs) + 1
    acts, refs = refs[:n_act], refs[n_act:]
    grads, refs = refs[:n_grad], refs[n_grad:]
    vec, refs = refs[0], refs[1:]
    outs, refs = refs[:n_out], refs[n_out:]
    vec_out, refs = refs[0], refs[1:]
    acts2, refs = refs[:n_act], refs[n_act:]
    grads2, refs = refs[:n_grad], refs[n_grad:]
    vec2, refs = refs[0], refs[1:]
    total = n_grad + 1
    sends = [refs[3 * m:3 * m + 3] for m in range(total)]
    refs = refs[3 * total:]
    comes = [refs[3 * m:3 * m + 3] for m in range(total)]
    refs = refs[3 * total:]
    keeps = {k.shape[1]: k for k in refs[:-4]}
    send, recv, swap_send, swap_recv = refs[-4:]
    place, core = place_of(sizes)
    base = slot_base(sizes)
    greet(sizes, place, core)
    started = []
    swaps = {}

    def swap(name, source, target):
        at = len(swaps)
        copy = pltpu.make_async_remote_copy(
            source, target, swap_send.at[at], swap_recv.at[at],
            device_id=device_of(sizes, place, 1 - core), device_id_type=MESH,
        )
        copy.start()
        swaps[name] = copy

    swap("vec", vec.at[1 - core], vec2)
    for m, job in enumerate(jobs):
        if ("a", job[0]) not in swaps:
            swap(("a", job[0]), acts[job[0]].at[1 - core], acts2[job[0]])
        swap(("g", m), grads[m], grads2[m])
    settled = set()

    def need(name):
        if name not in settled:
            settled.add(name)
            swaps[name].wait_recv()

    pending = []
    arrive = {}

    def flush(ready):
        for copy in ready:
            copy.start()
            started.append(copy)
            pending.remove(copy)

    def queue(m, phase, dim):
        waits = []
        for step in range(1, sizes[dim]):
            slot = base[dim] + step - 1
            copy = pltpu.make_async_remote_copy(
                sends[m][phase].at[step - 1], comes[m][phase].at[step - 1], send.at[m, slot], recv.at[m, slot],
                device_id=device_of(sizes, shifted(sizes, place, dim, step), core), device_id_type=MESH,
            )
            waits.append(copy)
        arrive[m, phase] = waits
        return waits

    def settle(m, phase):
        for copy in arrive[m, phase]:
            copy.wait_recv()

    def product(m, first, second, columns):
        act, act2, grad, grad2 = acts[jobs[m][0]], acts2[jobs[m][0]], grads[m], grads2[m]
        return jnp.dot(
            act[core, first, second], grad[:, columns], preferred_element_type=jnp.float32
        ) + jnp.dot(act2[first, second], grad2[:, columns], preferred_element_type=jnp.float32)

    def over_columns(width, body):
        @pl.loop(0, width // TILE)
        def _(i):
            body(pl.ds(pl.multiple_of(i * TILE, TILE), TILE))

    def work(m, phase):
        ready = list(pending)
        compute(m, phase)
        flush(ready)
        if phase < 3:
            pending.extend(queue(m, phase, jobs[m][4][phase]))

    def compute(m, phase):
        _, _, out, index, order, depth, width = jobs[m]
        d0, d1, d2 = order
        part = sizes[d2] * depth
        if phase == 0:
            need(("a", jobs[m][0]))
            need(("g", m))
            for step in range(1, sizes[d0]):
                there = lax.rem(place[d0] + step, sizes[d0])
                for second in range(sizes[d1]):
                    def body(columns, there=there, second=second, step=step):
                        value = product(m, there, second, columns)
                        sends[m][0][step - 1, second * part:(second + 1) * part, columns] = value.astype(jnp.bfloat16)
                    over_columns(width, body)
        elif phase == 1:
            settle(m, 0)
            for step in range(1, sizes[d1]):
                there = lax.rem(place[d1] + step, sizes[d1])
                rows = pl.ds(pl.multiple_of(there * part, 16), part)
                def body(columns, there=there, rows=rows, step=step):
                    value = product(m, place[d0], there, columns)
                    for other in range(sizes[d0] - 1):
                        value += comes[m][0][other, rows, columns].astype(jnp.float32)
                    sends[m][1][step - 1, :, columns] = value.astype(jnp.bfloat16)
                over_columns(width, body)
        elif phase == 2:
            settle(m, 1)
            rows = pl.ds(pl.multiple_of(place[d1] * part, 16), part)
            keep = keeps[width]
            def body(columns):
                value = product(m, place[d0], place[d1], columns)
                for other in range(sizes[d0] - 1):
                    value += comes[m][0][other, rows, columns].astype(jnp.float32)
                for other in range(sizes[d1] - 1):
                    value += comes[m][1][other, :, columns].astype(jnp.float32)
                keep[:part, columns] = value
                for step in range(1, sizes[d2]):
                    there = pl.ds(pl.multiple_of(lax.rem(place[d2] + step, sizes[d2]) * depth, 8), depth)
                    sends[m][2][step - 1, :, columns] = keep[there, columns].astype(jnp.bfloat16)
                here = pl.ds(pl.multiple_of(place[d2] * depth, 8), depth)
                target = outs[out] if index is None else outs[out].at[index]
                target[:, columns] = keep[here, columns]
            over_columns(width, body)
        else:
            settle(m, 2)
            target = outs[out] if index is None else outs[out].at[index]
            def body(columns):
                value = target[:, columns]
                for other in range(sizes[d2] - 1):
                    value += comes[m][2][other, :, columns].astype(jnp.float32)
                target[:, columns] = value
            over_columns(width, body)

    last = n_grad

    def vec_work(phase):
        d0, d1, d2 = FIRST[0]
        if phase == 0:
            need("vec")
            vec2[...] = vec2[...] + vec[core]
            for step in range(1, sizes[d0]):
                sends[last][0][step - 1] = vec2[lax.rem(place[d0] + step, sizes[d0])]
        elif phase == 1:
            settle(last, 0)
            value = vec2[place[d0]]
            for other in range(sizes[d0] - 1):
                value += comes[last][0][other]
            vec2[place[d0]] = value
            for step in range(1, sizes[d1]):
                sends[last][1][step - 1] = vec2[place[d0], lax.rem(place[d1] + step, sizes[d1])]
        elif phase == 2:
            settle(last, 1)
            value = vec2[place[d0], place[d1]]
            for other in range(sizes[d1] - 1):
                value += comes[last][1][other]
            vec2[place[d0], place[d1]] = value
            for step in range(1, sizes[d2]):
                sends[last][2][step - 1] = vec2[place[d0], place[d1], lax.rem(place[d2] + step, sizes[d2])]
        else:
            settle(last, 2)
            value = vec2[place[d0], place[d1], place[d2]]
            for other in range(sizes[d2] - 1):
                value += comes[last][2][other]
            vec_out[...] = value
        if phase < 3:
            pending.extend(queue(last, phase, FIRST[0][phase]))

    lag = 2
    for s in range(n_grad + 3 * lag):
        for phase in (3, 2, 1, 0):
            m = s - lag * phase
            if 0 <= m < n_grad:
                work(m, phase)
        if s < 4 * lag and s % lag == 0:
            vec_work(s // lag)
    flush(list(pending))
    for copy in started:
        copy.wait_send()
    for copy in swaps.values():
        copy.wait_send()


def scatter(sizes, acts, jobs, grads, vec, collective_id=1):
    n_act, total = len(acts), len(jobs) + 1
    X, Y, Z = sizes
    vmem = pl.BlockSpec(memory_space=pltpu.VMEM)
    shapes = {}
    for _, _, out, index, _, depth, width in jobs:
        shapes[out] = (depth, width) if index is None else (3, depth, width)
    outs = [jax.ShapeDtypeStruct(shapes[k], jnp.float32) for k in sorted(shapes)]
    outs.append(jax.ShapeDtypeStruct(vec.shape[4:], jnp.float32))
    scratch = [pltpu.VMEM(a.shape[1:], a.dtype) for a in acts]
    scratch += [pltpu.VMEM(g.shape, g.dtype) for g in grads]
    scratch.append(pltpu.VMEM(vec.shape[1:], jnp.float32))
    stages, keeps = [], {}
    for _, _, _, _, order, depth, width in jobs:
        a, b, c = (sizes[d] for d in order)
        stages += [
            pltpu.VMEM((a - 1, b * c * depth, width), jnp.bfloat16),
            pltpu.VMEM((b - 1, c * depth, width), jnp.bfloat16),
            pltpu.VMEM((c - 1, depth, width), jnp.bfloat16),
        ]
        keeps[width] = max(keeps.get(width, 0), c * depth)
    a, b, c = (sizes[d] for d in FIRST[0])
    tail = vec.shape[4:]
    stages += [
        pltpu.VMEM((a - 1, b, c, *tail), jnp.float32),
        pltpu.VMEM((b - 1, c, *tail), jnp.float32),
        pltpu.VMEM((c - 1, *tail), jnp.float32),
    ]
    scratch += stages + stages
    scratch += [pltpu.VMEM((rows, width), jnp.float32) for width, rows in sorted(keeps.items())]
    slots = sum(sizes) - 3
    swaps = 1 + len(grads) + len({j[0] for j in jobs})
    scratch += [pltpu.SemaphoreType.DMA((total, slots))] * 2 + [pltpu.SemaphoreType.DMA((swaps,))] * 2
    return pl.pallas_call(
        functools.partial(scatter_kernel, sizes, jobs, n_act),
        out_shape=outs,
        in_specs=[vmem] * (n_act + len(grads) + 1),
        out_specs=[vmem] * len(outs),
        scratch_shapes=scratch,
        compiler_params=pltpu.CompilerParams(
            collective_id=collective_id, has_side_effects=True, vmem_limit_bytes=66000000
        ),
    )(*acts, *grads, vec)


def padded(count):
    return -(-count // 16) * 16


def reduce_all(sizes, work, small_grads):
    X, Y, Z = sizes
    devices = 2 * X * Y * Z
    sums = [jnp.concatenate([jnp.atleast_2d(a).reshape(-1, devices, a.shape[-1] // devices).transpose(1, 0, 2).reshape(devices, -1) for a in small_grads], 1)]
    vec = jnp.pad(sums[0], ((0, 0), (0, 1024 - sums[0].shape[1])))
    depths = [a.shape[1] // devices for a, _, _ in work]
    if any(d % 8 or d * Z % 16 for d in depths):
        axes = ("gx", "gy")
        results = []
        for a, gs, _ in work:
            for_each = [
                lax.psum_scatter(
                    lax.dot_general(a, g, (((0,), (0,)), ((), ())), preferred_element_type=jnp.float32).astype(jnp.bfloat16),
                    axes, scatter_dimension=0, tiled=True,
                ).astype(jnp.float32)
                for g in gs
            ]
            results.append(for_each[0] if len(gs) == 1 else jnp.stack(for_each))
        vec_sum = lax.psum_scatter(vec, axes, scatter_dimension=0, tiled=True).reshape(-1)
    else:
        acts, jobs, grads = [], [], []
        for position, (a, gs, kind) in enumerate(work):
            rows = padded(a.shape[0])
            acts.append(arrange(sizes, FIRST[kind], a, rows))
            for index, g in enumerate(gs):
                jobs.append((
                    position, len(grads), position, index if len(gs) > 1 else None,
                    FIRST[kind], a.shape[1] // devices, g.shape[1],
                ))
                grads.append(jnp.pad(g, ((0, rows - g.shape[0]), (0, 0))))
        first, second, third = (block_axis(d) for d in FIRST[0])
        vec = vec.reshape(X, 2, Z, Y, 8, 128).transpose(1, first, second, third, 4, 5)
        results = scatter(sizes, acts, tuple(jobs), grads, vec)
        results, vec_sum = results[:-1], results[-1].reshape(-1)
    smalls, at = [], 0
    for a in small_grads:
        count = a.size // devices
        part = vec_sum[at:at + count]
        smalls.append(part if a.ndim == 1 else part.reshape(a.shape[0], -1))
        at += count
    return results, smalls


HT = 12
HV = 8
CHN = 8


EPSILON = 1e-06
MASKED = -30000.0
ROOT_HALF = 0.7071067811865476


def layer_norm(values, scale_gain, offset):
    center = values - jnp.mean(values, -1, keepdims=True)
    spread = jnp.mean(center * center, -1, keepdims=True)
    return center * lax.rsqrt(spread + EPSILON) * scale_gain + offset


def gelu_exact(values):
    return 0.5 * values * (1.0 + lax.erf(values * ROOT_HALF))


def project(inputs, weight):
    return jnp.dot(inputs, weight, preferred_element_type=jnp.float32)


def linear_back(inputs, weight, grad_low):
    input_grad = lax.dot_general(
        grad_low, weight, (((1,), (1,)), ((), ())), preferred_element_type=jnp.float32
    )
    bias_grad = jnp.sum(grad_low.astype(jnp.float32), 0)
    return (grad_low, bias_grad, input_grad)


def split_heads(values, pair_count, head_count):
    row_count, feature_width = values.shape
    return values.reshape(
        pair_count, row_count // pair_count, head_count, feature_width // head_count
    )


def attention_scores(queries, key_rows, key_live, head_count, pair_count):
    query_heads = split_heads(queries, pair_count, head_count)
    key_heads = split_heads(key_rows, pair_count, head_count)
    score_scale = (queries.shape[1] // head_count) ** (-0.5)
    scores = (
        jnp.einsum("pqhd,pkhd->phqk", query_heads, key_heads, preferred_element_type=jnp.float32)
        * score_scale
    )
    return scores + jnp.where(key_live[:, None, None, :], 0.0, MASKED)


def attend_forward(queries, key_rows, values, key_live, head_count, pair_count):
    scores = attention_scores(queries, key_rows, key_live, head_count, pair_count)
    row_max = jnp.max(scores, -1, keepdims=True)
    log_total = row_max + jnp.log(jnp.sum(jnp.exp(scores - row_max), -1, keepdims=True))
    attention = jnp.exp(scores - log_total).astype(jnp.bfloat16)
    value_heads = split_heads(values, pair_count, head_count)
    mixture = jnp.einsum(
        "phqk,pkhd->pqhd", attention, value_heads, preferred_element_type=jnp.float32
    )
    return (mixture.reshape(queries.shape[0], values.shape[1]).astype(jnp.bfloat16), log_total)


def attend_backward(
    queries, key_rows, values, key_live, head_count, pair_count, log_total, grad_low
):
    scores = attention_scores(queries, key_rows, key_live, head_count, pair_count)
    attention = jnp.exp(scores - log_total)
    attention_low = attention.astype(jnp.bfloat16)
    query_heads = split_heads(queries, pair_count, head_count)
    key_heads = split_heads(key_rows, pair_count, head_count)
    value_heads = split_heads(values, pair_count, head_count)
    grad_heads = split_heads(grad_low, pair_count, head_count)
    value_grad = jnp.einsum(
        "phqk,pqhd->pkhd", attention_low, grad_heads, preferred_element_type=jnp.float32
    )
    attention_grad = jnp.einsum(
        "pqhd,pkhd->phqk", grad_heads, value_heads, preferred_element_type=jnp.float32
    )
    score_grad = (
        attention * (attention_grad - jnp.sum(attention * attention_grad, -1, keepdims=True))
    ).astype(jnp.bfloat16)
    score_scale = (queries.shape[1] // head_count) ** (-0.5)
    query_grad = (
        jnp.einsum("phqk,pkhd->pqhd", score_grad, key_heads, preferred_element_type=jnp.float32)
        * score_scale
    )
    key_grad = (
        jnp.einsum("phqk,pqhd->pkhd", score_grad, query_heads, preferred_element_type=jnp.float32)
        * score_scale
    )
    return (
        query_grad.reshape(queries.shape).astype(jnp.bfloat16),
        key_grad.reshape(key_rows.shape).astype(jnp.bfloat16),
        value_grad.reshape(values.shape).astype(jnp.bfloat16),
    )


def projections_back(inputs, weights, grads):
    outcomes = [linear_back(inputs, weights[position], grads[position]) for position in range(3)]
    stacked = tuple(grads)
    input_grad = outcomes[0][2] + outcomes[1][2] + outcomes[2][2]
    return (stacked, outcomes[0][1], outcomes[2][1], input_grad)


def feed_forward(normed, up_weight, up_bias, down_weight, down_bias, scale_gain, offset):
    normed_low = normed.astype(jnp.bfloat16)
    pre_act = project(normed_low, up_weight) + up_bias
    hidden, gelu_back = jax.vjp(gelu_exact, pre_act)
    hidden_low = hidden.astype(jnp.bfloat16)
    branch = project(hidden_low, down_weight) + down_bias
    second, norm_back = jax.vjp(layer_norm, normed + branch, scale_gain, offset)
    return (second, (normed_low, hidden_low, gelu_back, norm_back))


def feed_back(kept, up_weight, down_weight, grad_second):
    normed_low, hidden_low, gelu_back, norm_back = kept
    pre_grad, gain_grad, shift_grad = norm_back(grad_second)
    down_grad, down_bias_grad, hidden_grad = linear_back(
        hidden_low, down_weight, pre_grad.astype(jnp.bfloat16)
    )
    (act_grad,) = gelu_back(hidden_grad)
    up_grad, up_bias_grad, normed_grad = linear_back(
        normed_low, up_weight, act_grad.astype(jnp.bfloat16)
    )
    return (
        up_grad,
        up_bias_grad,
        down_grad,
        down_bias_grad,
        gain_grad,
        shift_grad,
        pre_grad + normed_grad,
    )


def self_block(
    second, qkv_weight, out_weight, vectors, scale_gain, key_live, head_count, pair_count
):
    second_low = second.astype(jnp.bfloat16)
    queries = (project(second_low, qkv_weight[0]) + vectors[2]).astype(jnp.bfloat16)
    key_rows = project(second_low, qkv_weight[1]).astype(jnp.bfloat16)
    values = (project(second_low, qkv_weight[2]) + vectors[3]).astype(jnp.bfloat16)
    mixture, log_total = attend_forward(queries, key_rows, values, key_live, head_count, pair_count)
    final, norm_back = jax.vjp(
        layer_norm, second + project(mixture, out_weight) + vectors[4], scale_gain, vectors[7]
    )
    return (final, (second_low, queries, key_rows, values, mixture, log_total, norm_back))


def self_back(kept, qkv_weight, out_weight, key_live, head_count, pair_count, grad_final):
    second_low, queries, key_rows, values, mixture, log_total, norm_back = kept
    pre_grad, gain_grad, shift_grad = norm_back(grad_final)
    out_grad, out_bias_grad, mixture_grad = linear_back(
        mixture, out_weight, pre_grad.astype(jnp.bfloat16)
    )
    query_grad, key_grad, value_grad = attend_backward(
        queries,
        key_rows,
        values,
        key_live,
        head_count,
        pair_count,
        log_total,
        mixture_grad.astype(jnp.bfloat16),
    )
    qkv_grad, query_bias_grad, value_bias_grad, input_grad = projections_back(
        second_low, qkv_weight, (query_grad, key_grad, value_grad)
    )
    return (
        qkv_grad,
        out_grad,
        query_bias_grad,
        value_bias_grad,
        out_bias_grad,
        gain_grad,
        shift_grad,
        pre_grad + input_grad,
    )


def per_device(
    sizes,
    text_in,
    image_in,
    text_lengths,
    region_mask,
    text_cot,
    image_cot,
    co_text_proj,
    co_image_proj,
    co_bias,
    co_text_out,
    co_image_out,
    text_up,
    text_up_bias,
    text_down,
    image_up,
    image_up_bias,
    image_down,
    text_self_qkv,
    text_self_out,
    image_self_qkv,
    image_self_out,
    text_gains,
    image_gains,
    text_vectors,
    image_vectors,
):
    pair_count, text_len, text_width = text_in.shape
    region_count = image_in.shape[1]
    image_width = image_in.shape[2]
    text_rows = text_in.reshape(pair_count * text_len, text_width)
    image_rows = image_in.reshape(pair_count * region_count, image_width)
    text_live = lax.broadcasted_iota(jnp.int32, (pair_count, text_len), 1) < text_lengths[:, None]
    region_live = region_mask > 0
    small = (co_bias, text_gains, image_gains, text_vectors, image_vectors, text_up_bias, image_up_bias)
    big = (
        co_text_proj, co_image_proj, co_text_out, co_image_out, text_up, text_down, image_up, image_down,
        text_self_qkv, text_self_out, image_self_qkv, image_self_out,
    )
    full = gather_all(sizes, pack_small(small), big)
    (
        cross_bias_all, text_gain_all, image_gain_all, text_vector_all, image_vector_all,
        text_up_bias_all, image_up_bias_all,
    ) = unpack_small(full[0], small)
    text_proj_all, image_proj_all = full[1:4], full[4:7]
    text_out_all, image_out_all = full[7], full[8]
    feed_full = (full[9], text_up_bias_all, full[10], full[11], image_up_bias_all, full[12])
    self_full = (full[13:16], full[16], full[17:20], full[20])
    cross_bias_float = cross_bias_all.astype(jnp.float32)
    text_gain_float = text_gain_all.astype(jnp.float32)
    image_gain_float = image_gain_all.astype(jnp.float32)
    text_vector_float = text_vector_all.astype(jnp.float32)
    image_vector_float = image_vector_all.astype(jnp.float32)
    text_query = (project(text_rows, text_proj_all[0]) + cross_bias_float[0]).astype(jnp.bfloat16)
    text_key = project(text_rows, text_proj_all[1]).astype(jnp.bfloat16)
    text_value = (project(text_rows, text_proj_all[2]) + cross_bias_float[1]).astype(jnp.bfloat16)
    image_query = (project(image_rows, image_proj_all[0]) + cross_bias_float[2]).astype(
        jnp.bfloat16
    )
    image_key = project(image_rows, image_proj_all[1]).astype(jnp.bfloat16)
    image_value = (project(image_rows, image_proj_all[2]) + cross_bias_float[3]).astype(
        jnp.bfloat16
    )
    text_mixture, text_log = attend_forward(
        text_query, image_key, image_value, region_live, CHN, pair_count
    )
    image_mixture, image_log = attend_forward(
        image_query, text_key, text_value, text_live, CHN, pair_count
    )
    text_normed, text_norm_back = jax.vjp(
        layer_norm,
        text_rows.astype(jnp.float32) + project(text_mixture, text_out_all) + text_vector_float[0],
        text_gain_float[0],
        text_vector_float[5],
    )
    image_normed, image_norm_back = jax.vjp(
        layer_norm,
        image_rows.astype(jnp.float32)
        + project(image_mixture, image_out_all)
        + image_vector_float[0],
        image_gain_float[0],
        image_vector_float[5],
    )
    text_second, text_feed_kept = feed_forward(
        text_normed,
        feed_full[0],
        feed_full[1].astype(jnp.float32),
        feed_full[2],
        text_vector_float[1],
        text_gain_float[1],
        text_vector_float[6],
    )
    image_second, image_feed_kept = feed_forward(
        image_normed,
        feed_full[3],
        feed_full[4].astype(jnp.float32),
        feed_full[5],
        image_vector_float[1],
        image_gain_float[1],
        image_vector_float[6],
    )
    text_final, text_self_kept = self_block(
        text_second,
        self_full[0],
        self_full[1],
        text_vector_float,
        text_gain_float[2],
        text_live,
        HT,
        pair_count,
    )
    image_final, image_self_kept = self_block(
        image_second,
        self_full[2],
        self_full[3],
        image_vector_float,
        image_gain_float[2],
        region_live,
        HV,
        pair_count,
    )
    text_out = text_final.astype(jnp.bfloat16).reshape(pair_count, text_len, text_width)
    image_out = image_final.astype(jnp.bfloat16).reshape(pair_count, region_count, image_width)
    text_self_grads = self_back(
        text_self_kept,
        self_full[0],
        self_full[1],
        text_live,
        HT,
        pair_count,
        text_cot.reshape(pair_count * text_len, text_width).astype(jnp.float32),
    )
    image_self_grads = self_back(
        image_self_kept,
        self_full[2],
        self_full[3],
        region_live,
        HV,
        pair_count,
        image_cot.reshape(pair_count * region_count, image_width).astype(jnp.float32),
    )
    text_feed_grads = feed_back(
        text_feed_kept, feed_full[0], feed_full[2], text_self_grads[7]
    )
    image_feed_grads = feed_back(
        image_feed_kept, feed_full[3], feed_full[5], image_self_grads[7]
    )
    text_pre_grad, text_first_gain_grad, text_first_shift_grad = text_norm_back(text_feed_grads[6])
    image_pre_grad, image_first_gain_grad, image_first_shift_grad = image_norm_back(
        image_feed_grads[6]
    )
    text_out_grad, text_out_bias_grad, text_mixture_grad = linear_back(
        text_mixture, text_out_all, text_pre_grad.astype(jnp.bfloat16)
    )
    image_out_grad, image_out_bias_grad, image_mixture_grad = linear_back(
        image_mixture, image_out_all, image_pre_grad.astype(jnp.bfloat16)
    )
    text_query_grad, image_key_grad, image_value_grad = attend_backward(
        text_query,
        image_key,
        image_value,
        region_live,
        CHN,
        pair_count,
        text_log,
        text_mixture_grad.astype(jnp.bfloat16),
    )
    image_query_grad, text_key_grad, text_value_grad = attend_backward(
        image_query,
        text_key,
        text_value,
        text_live,
        CHN,
        pair_count,
        image_log,
        image_mixture_grad.astype(jnp.bfloat16),
    )
    text_proj_grad, text_query_bias_grad, text_value_bias_grad, text_input_grad = projections_back(
        text_rows, text_proj_all, (text_query_grad, text_key_grad, text_value_grad)
    )
    image_proj_grad, image_query_bias_grad, image_value_bias_grad, image_input_grad = (
        projections_back(
            image_rows, image_proj_all, (image_query_grad, image_key_grad, image_value_grad)
        )
    )
    cross_bias_grad = jnp.stack(
        [text_query_bias_grad, text_value_bias_grad, image_query_bias_grad, image_value_bias_grad]
    )
    text_gains_grad = jnp.stack([text_first_gain_grad, text_feed_grads[4], text_self_grads[5]])
    image_gains_grad = jnp.stack([image_first_gain_grad, image_feed_grads[4], image_self_grads[5]])
    text_vectors_grad = jnp.stack(
        [
            text_out_bias_grad,
            text_feed_grads[3],
            text_self_grads[2],
            text_self_grads[3],
            text_self_grads[4],
            text_first_shift_grad,
            text_feed_grads[5],
            text_self_grads[6],
        ]
    )
    image_vectors_grad = jnp.stack(
        [
            image_out_bias_grad,
            image_feed_grads[3],
            image_self_grads[2],
            image_self_grads[3],
            image_self_grads[4],
            image_first_shift_grad,
            image_feed_grads[5],
            image_self_grads[6],
        ]
    )
    work = (
        (text_self_kept[4], (text_self_grads[1],), 1),
        (image_self_kept[4], (image_self_grads[1],), 0),
        (text_self_kept[0], text_self_grads[0], 0),
        (image_self_kept[0], image_self_grads[0], 1),
        (text_feed_kept[1], (text_feed_grads[2],), 1),
        (image_feed_kept[1], (image_feed_grads[2],), 0),
        (text_feed_kept[0], (text_feed_grads[0],), 0),
        (image_feed_kept[0], (image_feed_grads[0],), 0),
        (text_mixture, (text_out_grad,), 1),
        (image_mixture, (image_out_grad,), 1),
        (text_rows, text_proj_grad, 1),
        (image_rows, image_proj_grad, 0),
    )
    sums, smalls = reduce_all(
        sizes,
        work,
        (
            cross_bias_grad, text_gains_grad, image_gains_grad, text_vectors_grad, image_vectors_grad,
            text_feed_grads[1], image_feed_grads[1],
        ),
    )
    text_in_grad = (
        (text_pre_grad + text_input_grad)
        .astype(jnp.bfloat16)
        .reshape(pair_count, text_len, text_width)
    )
    image_in_grad = (
        (image_pre_grad + image_input_grad)
        .astype(jnp.bfloat16)
        .reshape(pair_count, region_count, image_width)
    )
    return (
        text_out,
        image_out,
        text_in_grad,
        image_in_grad,
        sums[10],
        sums[11],
        smalls[0],
        sums[8],
        sums[9],
        sums[6],
        smalls[5],
        sums[4],
        sums[7],
        smalls[6],
        sums[5],
        sums[2],
        sums[0],
        sums[3],
        sums[1],
        smalls[1],
        smalls[2],
        smalls[3],
        smalls[4],
    )


def solution(mesh):
    placed = (
        P(("gx", "gy"), None, None),
        P(("gx", "gy"), None, None),
        P(("gx", "gy")),
        P(("gx", "gy"), None),
        P(("gx", "gy"), None, None),
        P(("gx", "gy"), None, None),
        P(None, ("gx", "gy"), None),
        P(None, ("gx", "gy"), None),
        P(None, ("gx", "gy")),
        P(("gx", "gy"), None),
        P(("gx", "gy"), None),
        P(("gx", "gy"), None),
        P(("gx", "gy")),
        P(("gx", "gy"), None),
        P(("gx", "gy"), None),
        P(("gx", "gy")),
        P(("gx", "gy"), None),
        P(None, ("gx", "gy"), None),
        P(("gx", "gy"), None),
        P(None, ("gx", "gy"), None),
        P(("gx", "gy"), None),
        P(None, ("gx", "gy")),
        P(None, ("gx", "gy")),
        P(None, ("gx", "gy")),
        P(None, ("gx", "gy")),
    )
    return jax.shard_map(
        functools.partial(per_device, mesh_sizes(mesh)),
        mesh=mesh,
        in_specs=placed,
        out_specs=(
            P(("gx", "gy"), None, None),
            P(("gx", "gy"), None, None),
            P(("gx", "gy"), None, None),
            P(("gx", "gy"), None, None),
            P(None, ("gx", "gy"), None),
            P(None, ("gx", "gy"), None),
            P(None, ("gx", "gy")),
            P(("gx", "gy"), None),
            P(("gx", "gy"), None),
            P(("gx", "gy"), None),
            P(("gx", "gy")),
            P(("gx", "gy"), None),
            P(("gx", "gy"), None),
            P(("gx", "gy")),
            P(("gx", "gy"), None),
            P(None, ("gx", "gy"), None),
            P(("gx", "gy"), None),
            P(None, ("gx", "gy"), None),
            P(("gx", "gy"), None),
            P(None, ("gx", "gy")),
            P(None, ("gx", "gy")),
            P(None, ("gx", "gy")),
            P(None, ("gx", "gy")),
        ),
        check_vma=False,
    )
```
